128 devices in a mesh: rep: 4 (over z_hi, core), fsdp: 32 (over y, x, z_lo).
Axes of the slice: x: 4, y: 4, z: 4 (z_hi: 2, z_lo: 2; z = z_hi * 2 + z_lo), core: 2. Of those that a mesh axis runs over, the one named last changes fastest.
Arguments:
- inputs: bfloat16 [4, 1536, 3584], P('rep', 'fsdp'), may hold values from -6 to 6
- cotangent: bfloat16 [4, 1536, 3584], P('rep', 'fsdp'), may hold values from -6 to 6
- w_gate: bfloat16 [4, 3584, 14336], P('rep', None, 'fsdp'), may hold values from -6 to 6
- w_up: bfloat16 [4, 3584, 14336], P('rep', None, 'fsdp'), may hold values from -6 to 6
- w_down: bfloat16 [4, 14336, 3584], P('rep', 'fsdp'), may hold values from -6 to 6
- outer_params: float32 [14336, 3584], P('fsdp', 'rep'), may hold values from -6 to 6
- outer_moment: float32 [14336, 3584], P('fsdp', 'rep'), may hold values from -2 to 2
Outputs:
- new_gate: bfloat16 [4, 3584, 14336], P('rep', None, 'fsdp')
- new_up: bfloat16 [4, 3584, 14336], P('rep', None, 'fsdp')
- mixed_down: bfloat16 [4, 14336, 3584], P('rep', 'fsdp')
- new_outer: float32 [14336, 3584], P('fsdp', 'rep')
- new_moment: float32 [14336, 3584], P('fsdp', 'rep')
The draws below stay inside these ranges and needn't reach their ends.
All inputs are finite; a program needn't handle non-finite values.
Results may differ from the reference program's by a relative error of at most 0.0075.
Values may be sent and summed in bfloat16 or wider, within the bound.
No kernel may reach another device: no remote copies, remote signals or barrier semaphores. Data moves between devices by JAX's collectives and lax.ppermute only.
A program may use at most 128 MiB of HBM per device.

```python
import math
import jax
import jax.numpy as jnp
from jax import lax

D = 3584
FF = 14336
TOKENS = 1536
REPS = 4
N_REP = 4


def level_of(rng, extent, cuts, least, top_value):
    level, own = 1.0, jax.random.fold_in(rng, 6)
    for dim, blocks in cuts:
        steps = jnp.exp(jax.random.uniform(jax.random.fold_in(own, dim), (blocks,), jnp.float32, least / len(cuts), top_value / len(cuts)))
        level = level * jnp.repeat(steps, extent[dim] // blocks).reshape([-1 if axis == dim else 1 for axis in range(len(extent))])
    return level


def scatter_about(stream_key, dims, deviation, limit, cuts=(), dtype=jnp.bfloat16):
    drawn = jax.random.normal(stream_key, dims, jnp.float32) * deviation
    if len(cuts) > 0:
        drawn = level_of(stream_key, dims, cuts, -0.22, 0.18) * drawn
    return jnp.clip(drawn, min=-limit, max=limit).astype(dtype)


def setup_inputs(seed: int = 0) -> dict:
    key_list = jax.random.split(jax.random.key(seed), 8)
    inputs = scatter_about(key_list[0], (REPS, TOKENS, D), 1.0, 6.0, ((0, 4), (1, 32)))
    cotangent = scatter_about(key_list[1], (REPS, TOKENS, D), 1.0, 6.0, ((0, 4), (1, 32)))
    w_gate = scatter_about(key_list[2], (REPS, D, FF), 1.0, 6.0, ((0, 4), (2, 32)))
    w_up = scatter_about(key_list[3], (REPS, D, FF), 1.0, 6.0, ((0, 4), (2, 32)))
    w_down = scatter_about(key_list[4], (REPS, FF, D), 1.0, 6.0, ((0, 4), (1, 32)))
    outer_params = scatter_about(key_list[5], (FF, D), 1.0, 6.0, ((0, 32), (1, 4)), jnp.float32)
    outer_moment = scatter_about(key_list[6], (FF, D), 0.3, 2.0, ((0, 32), (1, 4)), jnp.float32)
    return dict(inputs=inputs, cotangent=cotangent, w_gate=w_gate, w_up=w_up, w_down=w_down, outer_params=outer_params, outer_moment=outer_moment)


step_rate = 2.0
outer_rate = 0.7
moment_keep = 0.9
mix_share = 0.5

def gelu_pair(gate):
    const = math.sqrt(2.0 / math.pi)
    inner = const * (gate + 0.044715 * gate * gate * gate)
    tangent = jnp.tanh(inner)
    active = 0.5 * gate * (1.0 + tangent)
    slope = 0.5 * (1.0 + tangent) + 0.5 * gate * (1.0 - tangent * tangent) * const * (1.0 + 3.0 * 0.044715 * gate * gate)
    return (active, slope)

def inner_step(packed):
    rows, grads_out, wgate, wupper, wdown = packed
    scale_in = D ** (-0.5)
    scale_mid = FF ** (-0.5)
    gate = jnp.dot(rows, wgate, preferred_element_type=jnp.float32) * scale_in
    lifted = jnp.dot(rows, wupper, preferred_element_type=jnp.float32) * scale_in
    active, slope = gelu_pair(gate)
    hidden = (active * lifted).astype(jnp.bfloat16)
    back = jnp.dot(grads_out, wdown.T, preferred_element_type=jnp.float32) * scale_mid
    d_gate = (back * lifted * slope).astype(jnp.bfloat16)
    d_up = (back * active).astype(jnp.bfloat16)
    g_gate = jnp.dot(rows.T, d_gate, preferred_element_type=jnp.float32) * scale_in
    g_up = jnp.dot(rows.T, d_up, preferred_element_type=jnp.float32) * scale_in
    g_down = jnp.dot(hidden.T, grads_out, preferred_element_type=jnp.float32) * scale_mid
    new_gate = (wgate.astype(jnp.float32) - step_rate * g_gate).astype(jnp.bfloat16)
    new_up = (wupper.astype(jnp.float32) - step_rate * g_up).astype(jnp.bfloat16)
    after_down = wdown.astype(jnp.float32) - step_rate * g_down
    return (new_gate, new_up, after_down)

def reference(inputs, cotangent, w_gate, w_up, w_down, outer_params, outer_moment):
    new_gate, new_up, after_down = lax.map(inner_step, (inputs, cotangent, w_gate, w_up, w_down))
    average = lax.optimization_barrier(jnp.sum(w_down.astype(jnp.float32), axis=0)) / N_REP
    delta = outer_params - average
    new_moment = moment_keep * outer_moment + delta
    new_outer = outer_params - outer_rate * (moment_keep * new_moment + delta)
    mixed_down = (mix_share * after_down + (1.0 - mix_share) * new_outer[None]).astype(jnp.bfloat16)
    return (new_gate, new_up, mixed_down, new_outer, new_moment)
```

```python
import functools
import math

import jax
import jax.numpy as jnp
from jax import lax
from jax.experimental import pallas as pl
from jax.experimental.pallas import tpu as pltpu
from jax.sharding import Mesh
from jax.sharding import PartitionSpec as P

D = 3584
FF = 14336

step_rate = 2.0
outer_rate = 0.7
moment_keep = 0.9
mix_share = 0.5

SCALE_IN = D ** (-0.5)
SCALE_MID = FF ** (-0.5)


NT = (((1,), (1,)), ((), ()))
NN = (((1,), (0,)), ((), ()))
f32 = jnp.float32
bf16 = jnp.bfloat16


def gelu_pair(gate):
    const = math.sqrt(2.0 / math.pi)
    square = gate * gate
    tangent = jnp.tanh(const * gate * (1.0 + 0.044715 * square))
    half = 0.5 * (1.0 + tangent)
    active = gate * half
    slope = half + 0.5 * gate * (1.0 - tangent * tangent) * const * (
        1.0 + 3.0 * 0.044715 * square
    )
    return active, slope


def piece_copies(refs, buf, sem):
    out, at = [], 0
    for ref in refs:
        n = ref.shape[0]
        out.append(pltpu.make_async_copy(ref, buf.at[pl.ds(at, n)], sem))
        at += n
    return out


def front_body(k, tiles, *refs):
    a_refs, b_refs = refs[:k], refs[k : 2 * k]
    wg_ref, wu_ref, wd_ref = refs[2 * k : 2 * k + 3]
    h_ref, dg_ref, du_ref = refs[2 * k + 3 : 2 * k + 6]
    xa, xb, wg, wu, wd, sems = refs[2 * k + 6 :]
    ca = piece_copies(a_refs, xa, sems.at[0])
    cb = piece_copies(b_refs, xb, sems.at[1])
    cg = pltpu.make_async_copy(wg_ref, wg, sems.at[2])
    cu = pltpu.make_async_copy(wu_ref, wu, sems.at[3])
    cd = pltpu.make_async_copy(wd_ref, wd, sems.at[4])
    for c in ca:
        c.start()
    cg.start()
    cu.start()
    for c in cb:
        c.start()
    cd.start()
    for c in ca:
        c.wait()
    cg.wait()
    for t, (at, n) in enumerate(tiles):
        rows = pl.ds(at, n)
        gate = lax.dot_general(wg[...], xa[rows, :], NT, preferred_element_type=f32) * SCALE_IN
        if t == 0:
            cu.wait()
        lifted = lax.dot_general(wu[...], xa[rows, :], NT, preferred_element_type=f32) * SCALE_IN
        if t == 0:
            for c in cb:
                c.wait()
            cd.wait()
        back = lax.dot_general(wd[...], xb[rows, :], NT, preferred_element_type=f32) * SCALE_MID
        active, slope = gelu_pair(gate)
        h_ref[:, at : at + n] = (active * lifted).astype(bf16)
        dg_ref[:, at : at + n] = (back * lifted * slope).astype(bf16)
        du_ref[:, at : at + n] = (back * active).astype(bf16)


def front(a_pieces, b_pieces, wg, wu, wd):
    k = len(a_pieces)
    n = sum(p.shape[0] for p in a_pieces)
    m = wg.shape[0]
    tiles, at = [], 0
    while at < n:
        size = min(256, n - at)
        tiles.append((at, size))
        at += size
    any_spec = pl.BlockSpec(memory_space=pl.ANY)
    vm = pl.BlockSpec(memory_space=pltpu.VMEM)
    out = jax.ShapeDtypeStruct((m, n), bf16)
    return pl.pallas_call(
        functools.partial(front_body, k, tuple(tiles)),
        out_shape=(out, out, out),
        in_specs=[any_spec] * (2 * k + 3),
        out_specs=(vm, vm, vm),
        scratch_shapes=[
            pltpu.VMEM((n, D), bf16),
            pltpu.VMEM((n, D), bf16),
            pltpu.VMEM((m, D), bf16),
            pltpu.VMEM((m, D), bf16),
            pltpu.VMEM((m, D), bf16),
            pltpu.SemaphoreType.DMA((5,)),
        ],
        compiler_params=pltpu.CompilerParams(vmem_limit_bytes=40 << 20),
        cost_estimate=pl.CostEstimate(
            flops=6 * m * n * D, transcendentals=m * n, bytes_accessed=4 * n * D + 6 * m * D
        ),
        name="front",
    )(*a_pieces, *b_pieces, wg, wu, wd)


TILE = 512


def grads_body(ks, ns, steps, *refs):
    k = sum(ks)
    g = len(ns)
    a_refs, b_refs = refs[:k], refs[k : 2 * k]
    p = 2 * k
    h_refs, dg_refs, du_refs = refs[p : p + g], refs[p + g : p + 2 * g], refs[p + 2 * g : p + 3 * g]
    p += 3 * g
    wg_ref, wu_ref, wd_ref, oa_ref, ng_ref, nu_ref, nd_ref, xa, xb, sems = refs[p:]
    i = pl.program_id(0)

    def copies(step, slot):
        cols = pl.ds(pl.multiple_of(step * TILE, TILE), TILE)
        out, at = [], 0
        for ar, br in zip(a_refs, b_refs):
            n = ar.shape[0]
            out.append(
                pltpu.make_async_copy(ar.at[:, cols], xa.at[slot, pl.ds(at, n)], sems.at[0, slot])
            )
            out.append(
                pltpu.make_async_copy(br.at[:, cols], xb.at[slot, pl.ds(at, n)], sems.at[1, slot])
            )
            at += n
        return out

    slot = lax.rem(i, 2)

    @pl.when(i == 0)
    def _():
        for c in copies(0, 0):
            c.start()

    @pl.when(i + 1 < steps)
    def _():
        for c in copies(i + 1, 1 - slot):
            c.start()

    for c in copies(i, slot):
        c.wait()

    def total(d_refs, x):
        acc, at = None, 0
        for d_ref, n in zip(d_refs, ns):
            part = lax.dot_general(
                d_ref[...], x[slot, at : at + n, :], NN, preferred_element_type=f32
            )
            acc = part if acc is None else acc + part
            at += n
        return acc

    ng_ref[...] = (
        wg_ref[...].astype(f32) - (step_rate * SCALE_IN) * total(dg_refs, xa)
    ).astype(bf16)
    nu_ref[...] = (
        wu_ref[...].astype(f32) - (step_rate * SCALE_IN) * total(du_refs, xa)
    ).astype(bf16)
    after = wd_ref[...].astype(f32) - (step_rate * SCALE_MID) * total(h_refs, xb)
    nd_ref[...] = (
        mix_share * after + (1.0 - mix_share) * oa_ref[...].astype(f32)
    ).astype(bf16)


def grads(groups, wg, wu, wd, outer_all):
    ks = tuple(len(g[0]) for g in groups)
    a_pieces = [x for g in groups for x in g[0]]
    b_pieces = [x for g in groups for x in g[1]]
    hs, dgs, dus = ([g[2][j] for g in groups] for j in range(3))
    ns = tuple(h.shape[1] for h in hs)
    n = sum(ns)
    m = wg.shape[0]
    steps = D // TILE
    any_spec = pl.BlockSpec(memory_space=pl.ANY)
    vm = pl.BlockSpec(memory_space=pltpu.VMEM)
    col = pl.BlockSpec((m, TILE), lambda i: (0, i))
    out = jax.ShapeDtypeStruct((m, D), bf16)
    return pl.pallas_call(
        functools.partial(grads_body, ks, ns, steps),
        grid=(steps,),
        out_shape=(out, out, out),
        in_specs=[any_spec] * (2 * sum(ks)) + [vm] * (3 * len(groups)) + [col] * 4,
        out_specs=(col, col, col),
        scratch_shapes=[
            pltpu.VMEM((2, n, TILE), bf16),
            pltpu.VMEM((2, n, TILE), bf16),
            pltpu.SemaphoreType.DMA((2, 2)),
        ],
        compiler_params=pltpu.CompilerParams(
            vmem_limit_bytes=40 << 20, dimension_semantics=("arbitrary",)
        ),
        cost_estimate=pl.CostEstimate(
            flops=6 * m * n * D, transcendentals=0, bytes_accessed=4 * n * D + 14 * m * D
        ),
        name="grads",
    )(*a_pieces, *b_pieces, *hs, *dgs, *dus, wg, wu, wd, outer_all)


def shift(x, axis, by, size):
    return lax.ppermute(x, axis, [(i, (i + by) % size) for i in range(size)])


def ring_gather(a, b, axis):
    a_left = shift(a, axis, 1, 4)
    b_right = shift(b, axis, -1, 4)
    a_right = shift(a, axis, -1, 4)
    b_left = shift(b, axis, 1, 4)
    a_far = shift(a_left, axis, 1, 4)
    b_far = shift(b_right, axis, -1, 4)
    return (a_left, a_right, a_far), (b_left, b_right, b_far)


def replica_sum(wdown):
    zh = lax.axis_index("zh")
    co = lax.axis_index("co")
    w = wdown.shape[1] // 4
    take = lambda x, j: lax.dynamic_slice_in_dim(x, j * w, w, 1)
    give = jnp.concatenate([take(wdown, 1 - co), take(wdown, 3 - co)], 1)
    got = shift(give, "co", 1, 2)
    other = take(wdown, (1 - zh) * 2 + co).astype(f32) + take(got, 1 - zh).astype(f32)
    mine = take(wdown, zh * 2 + co).astype(f32) + take(got, zh).astype(f32)
    return mine + shift(other.astype(bf16), "zh", 1, 2).astype(f32)


def replica_gather(x):
    zh = lax.axis_index("zh")
    co = lax.axis_index("co")
    far = shift(x, "zh", 1, 2)
    x2 = shift(x, "co", 1, 2)
    far2 = shift(far, "co", 1, 2)
    pick = lambda p, a, b: jnp.where(p, a, b)
    near0, near1 = pick(co == 0, x, x2), pick(co == 0, x2, x)
    far0, far1 = pick(co == 0, far, far2), pick(co == 0, far2, far)
    return jnp.concatenate(
        [
            pick(zh == 0, near0, far0),
            pick(zh == 0, near1, far1),
            pick(zh == 0, far0, near0),
            pick(zh == 0, far1, near1),
        ],
        1,
    )


def outer_update(outer_params, outer_moment, share, replicas):
    delta = outer_params - share / replicas
    new_moment = moment_keep * outer_moment + delta
    new_outer = outer_params - outer_rate * (moment_keep * new_moment + delta)
    return (new_outer, new_moment)


def per_device(inputs, cotangent, w_gate, w_up, w_down, outer_params, outer_moment):
    wgate = w_gate[0].T
    wupper = w_up[0].T
    wdown = w_down[0]
    half = inputs.shape[1] // 2
    colours = []
    for c, (first, second) in enumerate((("x", "y"), ("y", "x"))):
        a = inputs[0, c * half : (c + 1) * half]
        b = cotangent[0, c * half : (c + 1) * half]
        ga, gb = ring_gather(a, b, first)
        a4 = jnp.concatenate((a,) + ga, 0)
        b4 = jnp.concatenate((b,) + gb, 0)
        colours.append((a4, b4, second))
    share = replica_sum(wdown)
    near = [(a4, b4) for a4, b4, _ in colours]
    za = [shift(a4, "zl", 1, 2) for a4, _, _ in colours]
    zb = [shift(b4, "zl", 1, 2) for _, b4, _ in colours]
    early = [ring_gather(a4, b4, second) for a4, b4, second in colours]
    new_outer, new_moment = outer_update(outer_params, outer_moment, share, 4)
    outer_all = replica_gather(new_outer.astype(bf16))
    late = [ring_gather(x, y, c[2]) for x, y, c in zip(za, zb, colours)]

    def group(a_list, b_list):
        return (a_list, b_list, front(a_list, b_list, wgate, wupper, wdown))

    g1 = group(
        [p[0] for p in near] + [x for e in early for x in e[0]],
        [p[1] for p in near] + [x for e in early for x in e[1]],
    )
    g2 = group(
        za + [x for e in late for x in e[0][:2]],
        zb + [x for e in late for x in e[1][:2]],
    )
    g3 = group([e[0][2] for e in late], [e[1][2] for e in late])
    new_gate, new_up, mixed = grads((g1, g2, g3), wgate, wupper, wdown, outer_all)
    return (new_gate.T[None], new_up.T[None], mixed[None], new_outer, new_moment)


def solution(mesh):
    fine = Mesh(mesh.devices.reshape(2, 2, 4, 4, 2), ("zh", "co", "y", "x", "zl"))
    rep, fsdp = ("zh", "co"), ("y", "x", "zl")
    in_specs = (
        P(rep, fsdp, None),
        P(rep, fsdp, None),
        P(rep, None, fsdp),
        P(rep, None, fsdp),
        P(rep, fsdp, None),
        P(fsdp, rep),
        P(fsdp, rep),
    )
    out_specs = (
        P(rep, None, fsdp),
        P(rep, None, fsdp),
        P(rep, fsdp, None),
        P(fsdp, rep),
        P(fsdp, rep),
    )
    return jax.shard_map(
        per_device, mesh=fine, in_specs=in_specs, out_specs=out_specs, check_vma=False
    )
```
